256 devices in a mesh: lon: 32 (over x_hi, z, core), lat: 8 (over y, x_lo).
Axes of the slice: x: 4 (x_hi: 2, x_lo: 2; x = x_hi * 2 + x_lo), y: 4, z: 8, core: 2. Of those that a mesh axis runs over, the one named last changes fastest.
Arguments:
- tokens: bfloat16 [2, 96, 147456], P(None, 'lat', 'lon'), may hold values from -6 to 6
- cotangent: bfloat16 [2, 48, 147456], P(None, 'lat', 'lon'), may hold values from -6 to 6
- kinds_one: int32 [1, 16], P(None, 'lat'), may hold values from 0 to 7
- kinds_two: int32 [1, 8], P(None, 'lat'), may hold values from 0 to 7
- table_one: float32 [8, 6, 3312], replicated, may hold values from -2 to 260
- table_two: float32 [8, 12, 3312], replicated, may hold values from -2 to 260
- gain_one: float32 [192], replicated, may hold values from 0.1 to 1.9
- gain_merge: float32 [768], replicated, may hold values from 0.1 to 1.9
- gain_two: float32 [384], replicated, may hold values from 0.1 to 1.9
- qkv_one: bfloat16 [192, 576], replicated, may hold values from -0.4375 to 0.4375
- proj_one: bfloat16 [192, 192], replicated, may hold values from -0.4375 to 0.4375
- merge_weight: bfloat16 [768, 384], replicated, may hold values from -0.21875 to 0.21875
- qkv_two: bfloat16 [384, 1152], replicated, may hold values from -0.3125 to 0.3125
- proj_two: bfloat16 [384, 384], replicated, may hold values from -0.3125 to 0.3125
Outputs:
- result: bfloat16 [2, 48, 147456], P(None, 'lat', 'lon')
- d_tokens: bfloat16 [2, 96, 147456], P(None, 'lat', 'lon')
- grad_qkv_one: bfloat16 [192, 576], replicated
- grad_proj_one: bfloat16 [192, 192], replicated
- grad_merge: bfloat16 [768, 384], replicated
- grad_qkv_two: bfloat16 [384, 1152], replicated
- grad_proj_two: bfloat16 [384, 384], replicated
The draws below stay inside these ranges and needn't reach their ends.
All inputs are finite; a program needn't handle non-finite values.
Results may differ from the reference program's by a relative error of at most 0.025.
Values may be sent and summed in bfloat16 or wider, within the bound.
A program may use at most 128 MiB of HBM per device.

```python
import jax
import jax.numpy as jnp
import numpy as np
from jax import lax

C1 = 192
C2 = 384
HEADS1 = 6
HEADS2 = 12
WIN_Z = 2
WIN_LAT = 6
WIN_LON = 12
LEVELS = 2
TYPES = 8
RELS = 3312
H = 96
W = 768
H2 = 48
W2 = 384


def table_law(key, head_count, salt):
    own_key = jax.random.fold_in(key, salt)
    base_key = jax.random.fold_in(own_key, 11)
    values = jax.random.uniform(base_key, (TYPES, head_count, RELS), jnp.float32, -2.0, 2.0)
    return values


def draw_table_one(key, part):
    return table_law(key, HEADS1, 1)


def draw_table_two(key, part):
    return table_law(key, HEADS2, 2)


def with_ends(drawn, rng, low, largest):
    longest = drawn.shape.index(max(drawn.shape))
    spots = []
    for shift in (0, 1):
        where = [jax.random.randint(jax.random.fold_in(rng, axis), (), 0, length) for axis, length in enumerate(drawn.shape)]
        where[longest] = (where[longest] + shift) % drawn.shape[longest]
        spots.append(tuple(where))
    return drawn.at[spots[0]].set(low).at[spots[1]].set(largest)


def steps_of(stream_key, shape, split, smallest, top_value):
    def one(dim, shards_of):
        draws = jax.random.uniform(jax.random.fold_in(jax.random.fold_in(stream_key, 6), dim), (shards_of,), jnp.float32, smallest / len(split), top_value / len(split))
        return jnp.repeat(jnp.exp(draws), shape[dim] // shards_of).reshape((-1,) + (1,) * (len(shape) - dim - 1))

    level = one(*split[0])
    for cut in split[1:]:
        level = level * one(*cut)
    return level


def gaussian(rng, extent, scale, most, shards=(), held_as=jnp.bfloat16):
    values = jax.random.normal(rng, extent, jnp.float32) * scale
    if len(shards) > 0:
        values = steps_of(rng, extent, shards, -0.22, 0.18) * values
    return jnp.clip(values, min=-most, max=most).astype(held_as)


def setup_inputs(seed: int = 0) -> dict:
    arg_keys = jax.random.split(jax.random.key(seed), 15)
    return {
        "tokens": gaussian(arg_keys[0], (LEVELS, H, W * C1), 1.0, 6.0, ((1, 8), (2, 32))),
        "cotangent": gaussian(arg_keys[1], (LEVELS, H2, W2 * C2), 1.0, 6.0, ((1, 8), (2, 32))),
        "kinds_one": with_ends(jax.random.randint(arg_keys[2], (LEVELS // WIN_Z, H // WIN_LAT), 0, TYPES), jax.random.fold_in(arg_keys[2], 1), 0, TYPES - 1).astype(jnp.int32),
        "kinds_two": with_ends(jax.random.randint(arg_keys[3], (LEVELS // WIN_Z, H2 // WIN_LAT), 0, TYPES), jax.random.fold_in(arg_keys[3], 1), 0, TYPES - 1).astype(jnp.int32),
        "table_one": draw_table_one(jax.random.fold_in(arg_keys[14], 71), 0),
        "table_two": draw_table_two(jax.random.fold_in(arg_keys[14], 71), 0),
        "gain_one": jnp.clip(1.0 + 0.18 * jax.random.normal(arg_keys[6], (C1,), jnp.float32), 0.1, 1.9),
        "gain_merge": jnp.clip(1.0 + 0.18 * jax.random.normal(arg_keys[7], (4 * C1,), jnp.float32), 0.1, 1.9),
        "gain_two": jnp.clip(1.0 + 0.18 * jax.random.normal(arg_keys[8], (C2,), jnp.float32), 0.1, 1.9),
        "qkv_one": gaussian(arg_keys[9], (C1, 3 * C1), C1 ** -0.5, 0.4375),
        "proj_one": gaussian(arg_keys[10], (C1, C1), C1 ** -0.5, 0.4375),
        "merge_weight": gaussian(arg_keys[11], (4 * C1, C2), (4 * C1) ** -0.5, 0.21875),
        "qkv_two": gaussian(arg_keys[12], (C2, 3 * C2), C2 ** -0.5, 0.3125),
        "proj_two": gaussian(arg_keys[13], (C2, C2), C2 ** -0.5, 0.3125),
    }


norm_epsilon = 1e-05
grad_epsilon = 1e-06
masked_score = -1e+30

def relative_table():
    window_size = WIN_Z * WIN_LAT * WIN_LON
    positions = np.arange(window_size)
    level_at = positions // (WIN_LAT * WIN_LON)
    row_at = positions // WIN_LON % WIN_LAT
    col_at = positions % WIN_LON
    joined = (level_at[:, None] * WIN_Z + level_at[None, :]) * (WIN_LAT * WIN_LAT)
    joined = joined + row_at[:, None] * WIN_LAT + row_at[None, :]
    joined = joined * (2 * WIN_LON - 1) + col_at[:, None] - col_at[None, :] + WIN_LON - 1
    return joined.astype(np.int32)

def layer_norm(values, scaling):
    centre = lax.optimization_barrier(jnp.mean(values, axis=-1, keepdims=True))
    spread = values - centre
    second = lax.optimization_barrier(jnp.mean(spread * spread, axis=-1, keepdims=True))
    return spread * lax.rsqrt(second + norm_epsilon) * scaling

def to_windows(lattice):
    level_count, row_count, col_count = lattice.shape[:3]
    trailing = lattice.shape[3:]
    trailing_axes = tuple(range(6, 6 + len(trailing)))
    pieces = lattice.reshape((level_count // WIN_Z, WIN_Z, row_count // WIN_LAT, WIN_LAT, col_count // WIN_LON, WIN_LON) + trailing)
    pieces = pieces.transpose((0, 2, 4, 1, 3, 5) + trailing_axes)
    return pieces.reshape((level_count // WIN_Z, row_count // WIN_LAT, col_count // WIN_LON, WIN_Z * WIN_LAT * WIN_LON) + trailing)

def from_windows(blocks, level_count, row_count, col_count):
    trailing = blocks.shape[4:]
    trailing_axes = tuple(range(6, 6 + len(trailing)))
    pieces = blocks.reshape((level_count // WIN_Z, row_count // WIN_LAT, col_count // WIN_LON, WIN_Z, WIN_LAT, WIN_LON) + trailing)
    pieces = pieces.transpose((0, 3, 1, 4, 2, 5) + trailing_axes)
    return pieces.reshape((level_count, row_count, col_count) + trailing)

def region_codes(level_count, row_start, row_count, rows_all):
    level_index = jnp.arange(level_count, dtype=jnp.int32)
    level_part = (level_index >= level_count - WIN_Z).astype(jnp.int32) + (level_index >= level_count - WIN_Z // 2).astype(jnp.int32)
    row_index = row_start + jnp.arange(row_count, dtype=jnp.int32)
    row_part = (row_index >= rows_all - WIN_LAT).astype(jnp.int32) + (row_index >= rows_all - WIN_LAT // 2).astype(jnp.int32)
    return level_part[:, None] * 3 + row_part[None, :]

def attend(shifted, kind_ids, bias_table, scaling, w_qkv, w_proj, head_count, row_start, rows_all, probe_qkv, probe_proj):
    level_count, row_count, col_count, channel_count = shifted.shape
    head_size = channel_count // head_count
    base_values = shifted.astype(jnp.float32)
    normed = layer_norm(base_values, scaling).astype(jnp.bfloat16)
    flat_rows = normed.reshape(-1, channel_count)
    packed = (jnp.dot(flat_rows, w_qkv, preferred_element_type=jnp.float32) + probe_qkv).astype(jnp.bfloat16)
    packed = to_windows(packed.reshape(level_count, row_count, col_count, 3, head_count, head_size))
    query_rows = packed[..., 0, :, :].astype(jnp.float32)
    key_rows = packed[..., 1, :, :].astype(jnp.float32)
    value_rows = packed[..., 2, :, :].astype(jnp.float32)
    scores = jnp.einsum('abdqhe,abdkhe->abdhqk', query_rows, key_rows) * head_size ** (-0.5)
    chosen = bias_table[kind_ids]
    full_bias = jnp.take(chosen, relative_table(), axis=3)
    scores = scores + full_bias[:, :, None]
    region_ids = region_codes(level_count, row_start, row_count, rows_all)
    tag_values = jnp.broadcast_to(region_ids[:, :, None], (level_count, row_count, col_count)).astype(jnp.float32)
    window_tags = to_windows(tag_values)
    allowed = window_tags[..., :, None] == window_tags[..., None, :]
    scores = jnp.where(allowed[:, :, :, None], scores, masked_score)
    row_top = lax.optimization_barrier(jnp.max(scores, axis=-1, keepdims=True))
    weights = jnp.exp(scores - row_top)
    attn_weights = (weights / lax.optimization_barrier(jnp.sum(weights, axis=-1, keepdims=True))).astype(jnp.bfloat16)
    attended = jnp.einsum('abdhqk,abdkhe->abdqhe', attn_weights.astype(jnp.float32), value_rows).astype(jnp.bfloat16)
    merged_rows = from_windows(attended, level_count, row_count, col_count).reshape(-1, channel_count)
    result = base_values.reshape(-1, channel_count) + jnp.dot(merged_rows, w_proj, preferred_element_type=jnp.float32) + probe_proj
    return (result.astype(jnp.bfloat16).reshape(shifted.shape), (flat_rows, merged_rows))

def merge_tokens(level_one, scaling, w_merge, probe_merge):
    level_count, row_count, col_count, channel_count = level_one.shape
    grouped = level_one.reshape(level_count, row_count // 2, 2, col_count // 2, 2, channel_count)
    grouped = grouped.transpose(0, 1, 3, 2, 4, 5).reshape(level_count, row_count // 2, col_count // 2, 4 * channel_count)
    normed = layer_norm(grouped.astype(jnp.float32), scaling).astype(jnp.bfloat16)
    flat_rows = normed.reshape(-1, 4 * channel_count)
    merged = (jnp.dot(flat_rows, w_merge, preferred_element_type=jnp.float32) + probe_merge).astype(jnp.bfloat16)
    return (merged.reshape(level_count, row_count // 2, col_count // 2, w_merge.shape[1]), flat_rows)

def weight_grad(inputs, cot_rows):
    return lax.dot_general(inputs, cot_rows.astype(jnp.bfloat16), (((0,), (0,)), ((), ())), preferred_element_type=jnp.float32)

def normalized(gradient):
    scale_back = lax.rsqrt(jnp.mean(gradient * gradient) + grad_epsilon)
    return (gradient * scale_back).astype(jnp.bfloat16)

def band_split(array, band_rows):
    level_count, row_count = array.shape[:2]
    band_stack = array.reshape((level_count, row_count // band_rows, band_rows) + array.shape[2:])
    return jnp.moveaxis(band_stack, 1, 0)

def band_join(band_stack):
    joined = jnp.moveaxis(band_stack, 0, 1)
    return joined.reshape((joined.shape[0], joined.shape[1] * joined.shape[2]) + joined.shape[3:])

def roll_ahead(lattice):
    return jnp.roll(lattice, (-(WIN_Z // 2), -(WIN_LAT // 2), -(WIN_LON // 2)), (0, 1, 2))

def roll_behind(lattice):
    return jnp.roll(lattice, (WIN_Z // 2, WIN_LAT // 2, WIN_LON // 2), (0, 1, 2))

def level_forward(shifted, kind_ids, bias_table, scaling, w_qkv, w_proj, head_count):
    rows_all = shifted.shape[1]
    band_count = rows_all // WIN_LAT
    operands = (band_split(shifted, WIN_LAT), band_split(kind_ids, 1), jnp.arange(band_count, dtype=jnp.int32) * WIN_LAT)

    def one_band(band_args):
        band_piece, kind_band, band_start = band_args
        token_count = band_piece.shape[0] * band_piece.shape[1] * band_piece.shape[2]
        channel_count = band_piece.shape[3]
        result, saved = attend(band_piece, kind_band, bias_table, scaling, w_qkv, w_proj, head_count, band_start, rows_all, jnp.zeros((token_count, 3 * channel_count), jnp.float32), jnp.zeros((token_count, channel_count), jnp.float32))
        return result
    return band_join(lax.map(one_band, operands))

def level_backward(shifted, kind_ids, bias_table, scaling, w_qkv, w_proj, head_count, cot_lattice):
    rows_all = shifted.shape[1]
    band_count = rows_all // WIN_LAT
    operands = (band_split(shifted, WIN_LAT), band_split(kind_ids, 1), jnp.arange(band_count, dtype=jnp.int32) * WIN_LAT, band_split(cot_lattice, WIN_LAT))

    def one_band(running, band_args):
        band_piece, kind_band, band_start, cot_band = band_args
        token_count = band_piece.shape[0] * band_piece.shape[1] * band_piece.shape[2]
        channel_count = band_piece.shape[3]

        def forward(lattice, probe_qkv, probe_proj):
            return attend(lattice, kind_band, bias_table, scaling, w_qkv, w_proj, head_count, band_start, rows_all, probe_qkv, probe_proj)
        result, pullback, saved = jax.vjp(forward, band_piece, jnp.zeros((token_count, 3 * channel_count), jnp.float32), jnp.zeros((token_count, channel_count), jnp.float32), has_aux=True)
        d_piece, d_packed, d_out = pullback(cot_band)
        running = (running[0] + weight_grad(saved[0], d_packed), running[1] + weight_grad(saved[1], d_out))
        return (running, d_piece)
    start_sums = (jnp.zeros(w_qkv.shape, jnp.float32), jnp.zeros(w_proj.shape, jnp.float32))
    sums, d_pieces = lax.scan(one_band, start_sums, operands)
    return (sums, band_join(d_pieces))

def merge_forward(level_one, scaling, w_merge):

    def one_band(band_piece):
        token_count = band_piece.shape[0] * (band_piece.shape[1] // 2) * (band_piece.shape[2] // 2)
        merged, flat_rows = merge_tokens(band_piece, scaling, w_merge, jnp.zeros((token_count, w_merge.shape[1]), jnp.float32))
        return merged
    return band_join(lax.map(one_band, band_split(level_one, 2 * WIN_LAT)))

def merge_backward(level_one, scaling, w_merge, cot_lattice):
    operands = (band_split(level_one, 2 * WIN_LAT), band_split(cot_lattice, WIN_LAT))

    def one_band(running, band_args):
        band_piece, cot_band = band_args
        token_count = band_piece.shape[0] * (band_piece.shape[1] // 2) * (band_piece.shape[2] // 2)

        def forward(lattice, probe_merge):
            return merge_tokens(lattice, scaling, w_merge, probe_merge)
        merged, pullback, flat_rows = jax.vjp(forward, band_piece, jnp.zeros((token_count, w_merge.shape[1]), jnp.float32), has_aux=True)
        d_piece, d_probe = pullback(cot_band)
        return (running + weight_grad(flat_rows, d_probe), d_piece)
    total, d_pieces = lax.scan(one_band, jnp.zeros(w_merge.shape, jnp.float32), operands)
    return (total, band_join(d_pieces))

def reference(tokens, cotangent, kinds_one, kinds_two, table_one, table_two, gain_one, gain_merge, gain_two, qkv_one, proj_one, merge_weight, qkv_two, proj_two):
    lattice = tokens.reshape(LEVELS, H, W, C1)
    shifted_one = roll_ahead(lattice)
    block_one = level_forward(shifted_one, kinds_one, table_one, gain_one, qkv_one, proj_one, HEADS1)
    level_one = roll_behind(block_one)
    merged = merge_forward(level_one, gain_merge, merge_weight)
    shifted_two = roll_ahead(merged)
    block_two = level_forward(shifted_two, kinds_two, table_two, gain_two, qkv_two, proj_two, HEADS2)
    level_two = roll_behind(block_two)
    d_block_two = roll_ahead(cotangent.reshape(LEVELS, H2, W2, C2))
    sums_two, d_shift_two = level_backward(shifted_two, kinds_two, table_two, gain_two, qkv_two, proj_two, HEADS2, d_block_two)
    d_merged = roll_behind(d_shift_two)
    raw_merge, d_level_one = merge_backward(level_one, gain_merge, merge_weight, d_merged)
    d_block_one = roll_ahead(d_level_one)
    sums_one, d_shift_one = level_backward(shifted_one, kinds_one, table_one, gain_one, qkv_one, proj_one, HEADS1, d_block_one)
    d_tokens = roll_behind(d_shift_one)
    return (level_two.reshape(LEVELS, H2, W2 * C2), d_tokens.reshape(LEVELS, H, W * C1), normalized(sums_one[0]), normalized(sums_one[1]), normalized(raw_merge), normalized(sums_two[0]), normalized(sums_two[1]))
```

```python
import functools

import jax
import jax.numpy as jnp
import numpy as np
from jax import lax
from jax.experimental import pallas as pl
from jax.experimental.pallas import tpu as pltpu
from jax.sharding import PartitionSpec as P

MESH = pl.DeviceIdType.MESH
BF = jnp.bfloat16
F32 = jnp.float32

C1 = 192
C2 = 384
HEADS1 = 6
HEADS2 = 12
HEAD = 32
ROWS1, COLS1 = 12, 24
ROWS2, COLS2 = 6, 12
HALF_LAT, HALF_LON = 3, 6
BLOCK = 80
VALID = 72
SPAN = 138

norm_epsilon = 1e-05
grad_epsilon = 1e-06
masked_score = -1e30
score_scale = HEAD**-0.5

VM = pl.BlockSpec(memory_space=pltpu.VMEM)
SM = pl.BlockSpec(memory_space=pltpu.SMEM)


def params(**more):
    return pltpu.CompilerParams(vmem_limit_bytes=60 * 1024 * 1024, **more)


def zone_starts(rows, cols):
    sizes = [
        2 * (rows - HALF_LAT) * (cols - HALF_LON),
        2 * HALF_LAT * (cols - HALF_LON),
        2 * (rows - HALF_LAT) * HALF_LON,
        2 * HALF_LAT * HALF_LON,
    ]
    padded = [-(-size // 16) * 16 for size in sizes]
    starts = [sum(padded[:i]) for i in range(4)]
    return starts, padded


def group_index(rows, cols, z, r, c, moved):
    starts, _ = zone_starts(rows, cols)
    if moved:
        far_r, far_c = r >= rows - HALF_LAT, c >= cols - HALF_LON
        r_in = r - (rows - HALF_LAT) if far_r else r
        c_in = c - (cols - HALF_LON) if far_c else c
    else:
        far_r, far_c = r < HALF_LAT, c < HALF_LON
        r_in = r if far_r else r - HALF_LAT
        c_in = c if far_c else c - HALF_LON
    width = HALF_LON if far_c else cols - HALF_LON
    return starts[int(far_r) + 2 * int(far_c)] + (r_in * width + c_in) * 2 + z


def window_index(z, r, c):
    return (((r // 6) * 2 + c // 12) * 2 + z) * BLOCK + (r % 6) * 12 + c % 12


def merge_index(z, r, c):
    part = (r % 2) * 2 + c % 2
    return part * 2 * BLOCK + z * BLOCK + (r // 2) * 12 + c // 2


def order_rows():
    maps = np.full((16, 768), -1, np.int32)
    gi = functools.partial(group_index, ROWS1, COLS1)
    gj = functools.partial(group_index, ROWS2, COLS2)
    for z in range(2):
        for r in range(ROWS1):
            for c in range(COLS1):
                t = (c * 2 + z) * 16 + r
                t_other = (c * 2 + 1 - z) * 16 + r
                win = window_index(z, r, c)
                mer = merge_index(z, r, c)
                maps[0, t] = gi(z, r, c, False)
                maps[2, gi(z, r, c, True)] = window_index(1 - z, r, c)
                maps[3, win] = gi(z, r, c, False)
                maps[4, gi(z, r, c, True)] = mer
                maps[5, mer] = gi(z, r, c, True)
                maps[8, gi(z, r, c, False)] = win
                maps[9, win] = gi(z, r, c, True)
                maps[10, gi(z, r, c, False)] = t_other
        for r in range(ROWS2):
            for c in range(COLS2):
                t = (c * 2 + z) * 8 + r
                t_other = (c * 2 + 1 - z) * 8 + r
                n = z * BLOCK + r * 12 + c
                maps[1, t] = gj(z, r, c, False)
                maps[6, gj(z, r, c, True)] = (1 - z) * BLOCK + r * 12 + c
                maps[7, n] = gj(z, r, c, True)
                maps[11, gj(z, r, c, False)] = t_other
    return maps


MAPS = order_rows()
STARTS1, PADDED1 = zone_starts(ROWS1, COLS1)
STARTS2, PADDED2 = zone_starts(ROWS2, COLS2)
GROUP1 = sum(PADDED1)
GROUP2 = sum(PADDED2)
HALO1 = GROUP1 - PADDED1[0]
HALO2 = GROUP2 - PADDED2[0]
WIN1 = 8 * BLOCK
WIN2 = 2 * BLOCK


def reorder(maps_ref, which, rows, source):
    width = source.shape[0]
    target = maps_ref[which : which + 1, :width]
    chosen = lax.broadcasted_iota(jnp.int32, (rows, width), 0) == target
    one_hot = jnp.where(chosen, 1.0, 0.0).astype(BF)
    return jnp.dot(one_hot, source, preferred_element_type=F32)


def dot_t(a, b):
    return lax.dot_general(a, b, (((1,), (1,)), ((), ())), preferred_element_type=F32)


def t_dot(a, b):
    return lax.dot_general(a, b, (((0,), (0,)), ((), ())), preferred_element_type=F32)


def dot(a, b):
    return jnp.dot(a, b, preferred_element_type=F32)


def standard(x):
    centre = jnp.mean(x, axis=-1, keepdims=True)
    spread = x - centre
    second = jnp.mean(spread * spread, axis=-1, keepdims=True)
    rstd = lax.rsqrt(second + norm_epsilon)
    return spread * rstd, rstd


def head_stack(value, heads):
    lane_head = lax.broadcasted_iota(jnp.int32, value.shape, 1) // HEAD
    zero = jnp.zeros_like(value)
    return jnp.concatenate([jnp.where(lane_head == h, value, zero) for h in range(heads)], axis=0)


def head_join(stacked, heads):
    rows = stacked.shape[0] // heads
    lane_head = lax.broadcasted_iota(jnp.int32, (rows, stacked.shape[1]), 1) // HEAD
    total = jnp.zeros((rows, stacked.shape[1]), F32)
    for h in range(heads):
        total = jnp.where(lane_head == h, stacked[h * rows : (h + 1) * rows], total)
    return total


def attention_fwd(q, k, v, bias, heads):
    scores = dot_t(head_stack(q, heads), k) * score_scale + bias[:, :BLOCK]
    top = jnp.max(scores, axis=-1, keepdims=True)
    weights = jnp.exp(scores - top)
    probs = (weights / jnp.sum(weights, axis=-1, keepdims=True)).astype(BF)
    return probs, head_join(dot(probs, v), heads).astype(BF)


def attention_bwd(q, k, v, probs, d_att, heads):
    d_stack = head_stack(d_att, heads)
    d_probs = dot_t(d_stack, v)
    p = probs.astype(F32)
    weighted = p * d_probs
    d_scores = (weighted - p * jnp.sum(weighted, axis=-1, keepdims=True)).astype(BF)
    d_q = head_join(dot(d_scores, k), heads) * score_scale
    d_k = t_dot(d_scores, head_stack(q, heads)) * score_scale
    d_v = t_dot(probs, d_stack)
    return d_q.astype(BF), d_k.astype(BF), d_v.astype(BF)


def norm_bwd(dy_parts, hats, rstd, width):
    first = sum(jnp.sum(dy, axis=-1, keepdims=True) for dy in dy_parts) / width
    second = sum(jnp.sum(dy * hat, axis=-1, keepdims=True) for dy, hat in zip(dy_parts, hats)) / width
    return [rstd * (dy - first - hat * second) for dy, hat in zip(dy_parts, hats)]


def pack_kernel(maps_ref, tokens_ref, cot_ref, group_ref, cot_group_ref, rows_ref, cot_rows_ref):
    rows_ref[...] = jnp.zeros_like(rows_ref)
    cot_rows_ref[...] = jnp.zeros_like(cot_rows_ref)
    for z in range(2):
        level = tokens_ref[z].astype(F32)
        cot = cot_ref[z].astype(F32)
        for c in range(COLS1):
            start = (c * 2 + z) * 16
            rows_ref[start : start + ROWS1, :] = level[:, c * C1 : (c + 1) * C1]
        for c in range(COLS2):
            start = (c * 2 + z) * 8
            cot_rows_ref[start : start + ROWS2, :] = cot[:, c * C2 : (c + 1) * C2]
    group_ref[...] = reorder(maps_ref, 0, GROUP1, rows_ref[...].astype(BF)).astype(BF)
    cot_group_ref[...] = reorder(maps_ref, 1, GROUP2, cot_rows_ref[...].astype(BF)).astype(BF)


def bias_kernel(kinds1_ref, kinds2_ref, table1_ref, table2_ref, spread_ref, bias1_ref, bias2_ref, seg_ref, wide_ref):
    is_last = lax.axis_index("lat") == lax.axis_size("lat") - 1
    seg_ref[...] = jnp.zeros_like(seg_ref)
    jobs = [(table1_ref[kinds1_ref[0, band]], HEADS1, band == 1) for band in range(2)]
    jobs.append((table2_ref[kinds2_ref[0, 0]], HEADS2, True))
    base = 0
    plans = []
    for number, (table, heads, last_band) in enumerate(jobs):
        for z in range(2):
            for a in range(6):
                start = z * 2484 + a * SPAN
                seg_ref.at[0][pl.ds(base + a, heads, stride=8), :] = table[:, start : start + 128]
                seg_ref.at[1][pl.ds(base + a, heads, stride=8), :] = table[:, start + SPAN - 128 : start + SPAN]
            for h in range(heads):
                plans.append((number, z, h, last_band, base + h * 8))
            base += heads * 8
    segs = jnp.concatenate([seg_ref[0], seg_ref[1]], axis=1)
    high = segs.astype(BF)
    rest = segs - high.astype(F32)
    middle = rest.astype(BF)
    low = (rest - middle.astype(F32)).astype(BF)
    for b in range(12):
        spread = spread_ref[:, b * 128 : (b + 1) * 128]
        wide_ref[:, b * 128 : (b + 1) * 128] = dot(high, spread) + dot(middle, spread) + dot(low, spread)
    bias1_ref[...] = jnp.zeros_like(bias1_ref)
    bias2_ref[...] = jnp.zeros_like(bias2_ref)
    for number, z, h, last_band, row in plans:
        for b in range(12):
            piece = wide_ref[row : row + 6, b * 128 : (b + 1) * 128]
            if number < 2:
                bias1_ref.at[number * 2 + z][pl.ds(h * BLOCK + b, 6, stride=12), :] = piece
            else:
                bias2_ref.at[z][pl.ds(h * BLOCK + b, 6, stride=12), :] = piece
    for ref, which, heads in ((bias1_ref, (2, 3), HEADS1), (bias1_ref, (0, 1), HEADS1), (bias2_ref, (0, 1), HEADS2)):
        rows = heads * BLOCK
        key = lax.broadcasted_iota(jnp.int32, (rows, 128), 1)
        row = lax.broadcasted_iota(jnp.int32, (rows, 128), 0) % BLOCK
        blocked = key >= VALID
        if not (ref is bias1_ref and which == (0, 1)):
            blocked = blocked | (((key < 36) != (row < 36)) & is_last)
        for i in which:
            ref[i] = jnp.where(blocked, masked_score, ref[i])


def first_kernel(
    maps_ref, group_ref, halo_ref, bias_ref, gain_ref, qkv_ref, proj_ref,
    out_ref, x_ref, normed_ref, q_ref, k_ref, v_ref, probs_ref, att_ref,
):
    source = jnp.concatenate([group_ref[: PADDED1[0]], halo_ref[...]], axis=0)
    x = reorder(maps_ref, 2, WIN1, source)
    x_ref[...] = x.astype(BF)
    hat, _ = standard(x)
    normed = (hat * gain_ref[...]).astype(BF)
    normed_ref[...] = normed
    packed = dot(normed, qkv_ref[...]).astype(BF)
    q_ref[...] = packed[:, :C1]
    k_ref[...] = packed[:, C1 : 2 * C1]
    v_ref[...] = packed[:, 2 * C1 :]

    @pl.loop(0, 8)
    def _(block):
        here = pl.ds(pl.multiple_of(block * BLOCK, 16), BLOCK)
        bias = bias_ref[(block // 4) * 2 + block % 2]
        probs, att = attention_fwd(q_ref[here, :], k_ref[here, :], v_ref[here, :], bias, HEADS1)
        probs_ref[pl.ds(pl.multiple_of(block * BLOCK * HEADS1, 16), BLOCK * HEADS1), :] = probs
        att_ref[here, :] = att

    block_one = (x_ref[...].astype(F32) + dot(att_ref[...], proj_ref[...])).astype(BF)
    out_ref[...] = reorder(maps_ref, 3, GROUP1, block_one).astype(BF)


def put_tiles(ref, start, value):
    rows = value.shape[0]
    for j in range(value.shape[1] // 128):
        ref[start + j * rows : start + (j + 1) * rows, :] = value[:, j * 128 : (j + 1) * 128].astype(BF)


MERGE_AT = 0
QKV2_AT = 3 * 4 * C1
PROJ2_AT = QKV2_AT + 9 * C2
ONE_AT = PROJ2_AT + 3 * C2
SUM_ROWS = 8192
TOP_ROWS = ONE_AT


def middle_kernel(
    maps_ref, group_ref, halo_ref, cot_ref, cot_halo_ref, bias_ref, gain_merge_ref, gain_ref, merge_ref, qkv_ref,
    proj_ref, d_group_ref, result_ref, sums_ref, nm_ref, raw_ref,
):
    source = jnp.concatenate([group_ref[: PADDED1[0]], halo_ref[...]], axis=0)
    grouped = reorder(maps_ref, 4, 4 * WIN2, source)
    parts = [grouped[i * WIN2 : (i + 1) * WIN2] for i in range(4)]
    width = 4 * C1
    centre = sum(jnp.sum(part, axis=-1, keepdims=True) for part in parts) / width
    spreads = [part - centre for part in parts]
    second = sum(jnp.sum(s * s, axis=-1, keepdims=True) for s in spreads) / width
    rstd_m = lax.rsqrt(second + norm_epsilon)
    hats_m = [s * rstd_m for s in spreads]
    gains_m = [gain_merge_ref[:, i * C1 : (i + 1) * C1] for i in range(4)]
    weights_m = [merge_ref[i * C1 : (i + 1) * C1, :] for i in range(4)]
    merged = jnp.zeros((WIN2, C2), F32)
    for i in range(4):
        nm_ref[i] = (hats_m[i] * gains_m[i]).astype(BF)
        merged = merged + dot(nm_ref[i], weights_m[i])
    x2 = merged.astype(BF).astype(F32)
    hat2, rstd2 = standard(x2)
    normed2 = (hat2 * gain_ref[...]).astype(BF)
    packed2 = dot(normed2, qkv_ref[...]).astype(BF)

    saved = []
    for z in range(2):
        rows = packed2[z * BLOCK : (z + 1) * BLOCK]
        q, k, v = rows[:, :C2], rows[:, C2 : 2 * C2], rows[:, 2 * C2 :]
        probs, att = attention_fwd(q, k, v, bias_ref[z], HEADS2)
        saved.append((q, k, v, probs, att))
    att2 = jnp.concatenate([s[4] for s in saved], axis=0)
    block_two = (x2 + dot(att2, proj_ref[...])).astype(BF)
    result_ref[...] = reorder(maps_ref, 7, GROUP2, block_two).astype(BF)

    cot_source = jnp.concatenate([cot_ref[: PADDED2[0]], cot_halo_ref[...]], axis=0)
    d_out = reorder(maps_ref, 6, WIN2, cot_source).astype(BF)
    raw_ref[:C2, :C2] = t_dot(att2, d_out)
    put_tiles(sums_ref, PROJ2_AT, raw_ref[:C2, :C2])
    d_att = dot_t(d_out, proj_ref[...]).astype(BF)
    pulled = []
    for z in range(2):
        q, k, v, probs, _ = saved[z]
        pulled.append(attention_bwd(q, k, v, probs, d_att[z * BLOCK : (z + 1) * BLOCK], HEADS2))
    d_packed = [jnp.concatenate([pulled[0][i], pulled[1][i]], axis=0) for i in range(3)]
    d_normed = jnp.zeros((WIN2, C2), F32)
    for i in range(3):
        put_tiles(sums_ref, QKV2_AT + 3 * i * C2, t_dot(normed2, d_packed[i]))
        d_normed = d_normed + dot_t(d_packed[i], qkv_ref[:, i * C2 : (i + 1) * C2])
    dy = d_normed.astype(BF).astype(F32) * gain_ref[...]
    d_x2 = d_out.astype(F32) + norm_bwd([dy], [hat2], rstd2, C2)[0]
    d_merged = d_x2.astype(BF)

    dys = []
    for i in range(4):
        raw_ref[i * C1 : (i + 1) * C1, :] = t_dot(nm_ref[i], d_merged)
        dys.append(dot_t(d_merged, weights_m[i]).astype(BF).astype(F32) * gains_m[i])
    put_tiles(sums_ref, MERGE_AT, raw_ref[...])
    d_parts = norm_bwd(dys, hats_m, rstd_m, width)
    d_grouped = jnp.concatenate([d.astype(BF) for d in d_parts], axis=0)
    d_group_ref[...] = reorder(maps_ref, 5, GROUP1, d_grouped).astype(BF)


def last_kernel(
    maps_ref, group_ref, halo_ref, gain_ref, qkv_ref, proj_ref, x_ref, normed_ref, q_ref, k_ref, v_ref, probs_ref,
    att_ref, sums_ref, d_group_ref, all_ref, d_att_ref, dq_ref, dk_ref, dv_ref,
):
    source = jnp.concatenate([group_ref[: PADDED1[0]], halo_ref[...]], axis=0)
    d_out = reorder(maps_ref, 8, WIN1, source).astype(BF)
    d_att_ref[...] = dot_t(d_out, proj_ref[...]).astype(BF)

    @pl.loop(0, 8)
    def _(block):
        here = pl.ds(pl.multiple_of(block * BLOCK, 16), BLOCK)
        probs = probs_ref[pl.ds(pl.multiple_of(block * BLOCK * HEADS1, 16), BLOCK * HEADS1), :]
        d_q, d_k, d_v = attention_bwd(q_ref[here, :], k_ref[here, :], v_ref[here, :], probs, d_att_ref[here, :], HEADS1)
        dq_ref[here, :] = d_q
        dk_ref[here, :] = d_k
        dv_ref[here, :] = d_v

    normed = normed_ref[...]
    d_packed = jnp.concatenate([dq_ref[...], dk_ref[...], dv_ref[...]], axis=1)
    raw_one = jnp.concatenate([t_dot(normed, d_packed), t_dot(att_ref[...], d_out)], axis=1)
    put_tiles(all_ref, ONE_AT, raw_one)
    all_ref[:TOP_ROWS, :] = sums_ref[...]
    all_ref[ONE_AT + 6 * C1 :, :] = jnp.zeros((SUM_ROWS - ONE_AT - 6 * C1, 128), BF)
    d_normed = dot_t(d_packed, qkv_ref[...])
    hat, rstd = standard(x_ref[...].astype(F32))
    dy = d_normed.astype(BF).astype(F32) * gain_ref[...]
    d_x = d_out.astype(F32) + norm_bwd([dy], [hat], rstd, C1)[0]
    d_group_ref[...] = reorder(maps_ref, 9, GROUP1, d_x.astype(BF)).astype(BF)


def final_kernel(
    maps_ref, d_group_ref, d_halo_ref, res_ref, res_halo_ref, sums_ref,
    result_ref, d_tokens_ref, qkv1_ref, proj1_ref, merge_ref, qkv2_ref, proj2_ref,
):
    source = jnp.concatenate([d_group_ref[: PADDED1[0]], d_halo_ref[...]], axis=0)
    rows = reorder(maps_ref, 10, 32 * COLS1, source)
    res_source = jnp.concatenate([res_ref[: PADDED2[0]], res_halo_ref[...]], axis=0)
    res_rows = reorder(maps_ref, 11, 16 * COLS2, res_source)
    for z in range(2):
        pieces = [rows[(c * 2 + z) * 16 : (c * 2 + z) * 16 + 16] for c in range(COLS1)]
        for c in range(0, COLS1, 2):
            pair = jnp.concatenate([pieces[c], pieces[c + 1]], axis=1).astype(BF)
            d_tokens_ref[z, :, c * C1 : (c + 2) * C1] = pair[:ROWS1]
        for c in range(COLS2):
            start = (c * 2 + z) * 8
            result_ref[z, :, c * C2 : (c + 1) * C2] = res_rows[start : start + 8].astype(BF)[:ROWS2]

    def section(start, rows, lanes):
        tiles = [sums_ref[start + j * rows : start + (j + 1) * rows, :].astype(F32) for j in range(lanes // 128)]
        return tiles

    def norm_scale(tiles, count):
        total = sum(jnp.sum(t * t, axis=0, keepdims=True) for t in tiles)
        total = jnp.sum(total, axis=1, keepdims=True)
        return lax.rsqrt(total / count + grad_epsilon)

    for ref, start, shape in ((merge_ref, MERGE_AT, (4 * C1, C2)), (qkv2_ref, QKV2_AT, (C2, 3 * C2)), (proj2_ref, PROJ2_AT, (C2, C2))):
        tiles = section(start, *shape)
        scale = norm_scale(tiles, shape[0] * shape[1])
        for j, tile in enumerate(tiles):
            ref[:, j * 128 : (j + 1) * 128] = (tile * scale).astype(BF)
    tiles = section(ONE_AT, C1, 4 * C1)
    halves = lax.broadcasted_iota(jnp.int32, (C1, 128), 1) < 64
    zero = jnp.zeros((C1, 128), F32)
    qkv_tiles = tiles[:4] + [jnp.where(halves, tiles[4], zero)]
    proj_tiles = [jnp.where(halves, zero, tiles[4]), tiles[5]]
    scale = norm_scale(qkv_tiles, 3 * C1 * C1)
    for j in range(4):
        qkv1_ref[:, j * 128 : (j + 1) * 128] = (tiles[j] * scale).astype(BF)
    qkv1_ref[:, 512:576] = (tiles[4] * scale).astype(BF)[:, :64]
    scale = norm_scale(proj_tiles, C1 * C1)
    both = jnp.concatenate([tiles[4], tiles[5]], axis=1) * scale
    proj1_ref[...] = both[:, 64:].astype(BF)


def neighbour(steps_lat, steps_lon):
    lat, lon = lax.axis_index("lat"), lax.axis_index("lon")
    rows, cols = lax.axis_size("lat"), lax.axis_size("lon")
    return {"lat": lax.rem(lat + rows + steps_lat, rows), "lon": lax.rem(lon + cols + steps_lon, cols)}


ZONE_STEPS = ((1, 0), (0, 1), (1, 1))


def zone_copies(sources, targets, layouts, direction, send_sem, recv_sem):
    copies = []
    for source, target, (starts, padded) in zip(sources, targets, layouts):
        for i, (lat_step, lon_step) in enumerate(ZONE_STEPS):
            number = len(copies)
            copies.append(
                pltpu.make_async_remote_copy(
                    src_ref=source.at[pl.ds(starts[i + 1], padded[i + 1]), :],
                    dst_ref=target.at[pl.ds(starts[i + 1] - padded[0], padded[i + 1]), :],
                    send_sem=send_sem.at[number],
                    recv_sem=recv_sem.at[number],
                    device_id=neighbour(direction * lat_step, direction * lon_step),
                    device_id_type=MESH,
                )
            )
    return copies


LAYOUTS = ((STARTS1, PADDED1), (STARTS2, PADDED2))


def halo_kernel(direction, count, *refs):
    sources, targets, (send_sem, recv_sem) = refs[:count], refs[count : 2 * count], refs[2 * count :]
    barrier = pltpu.get_barrier_semaphore()
    for lat_step, lon_step in ZONE_STEPS:
        pl.semaphore_signal(
            barrier, inc=1, device_id=neighbour(-direction * lat_step, -direction * lon_step), device_id_type=MESH
        )
    pl.semaphore_wait(barrier, 3)
    copies = zone_copies(sources, targets, LAYOUTS, direction, send_sem, recv_sem)
    for copy in copies:
        copy.start()
    for copy in copies:
        copy.wait()


def halo(sources, direction, collective_id):
    count = len(sources)
    shapes = ((HALO1, C1), (HALO2, C2))[:count]
    return pl.pallas_call(
        functools.partial(halo_kernel, direction, count),
        out_shape=tuple(jax.ShapeDtypeStruct(shape, BF) for shape in shapes),
        in_specs=[VM] * count,
        out_specs=(VM,) * count,
        scratch_shapes=[pltpu.SemaphoreType.DMA((3 * count,)), pltpu.SemaphoreType.DMA((3 * count,))],
        compiler_params=params(collective_id=collective_id, has_side_effects=True),
    )(*sources)


def coordinates():
    lat, lon = lax.axis_index("lat"), lax.axis_index("lon")
    depth = lax.axis_size("lon") // 4
    return {
        "x": lax.div(lon, 2 * depth) * 2 + lax.rem(lat, 2),
        "y": lax.div(lat, 2),
        "z": lax.rem(lax.div(lon, 2), depth),
        "core": lax.rem(lon, 2),
    }


def axis_sizes():
    return {"x": 4, "y": lax.axis_size("lat") // 2, "z": lax.axis_size("lon") // 4, "core": 2}


def device_at(place):
    depth = lax.axis_size("lon") // 4
    lon = lax.div(place["x"], 2) * (2 * depth) + place["z"] * 2 + place["core"]
    return {"lat": place["y"] * 2 + lax.rem(place["x"], 2), "lon": lon}


ROUTES = (("x", "y", "z"), ("y", "x", "z"))
PART_ROWS = SUM_ROWS // 2
CORE_ROWS = PART_ROWS // 2


def sum_kernel(
    sums_ref, d_ref, out_ref, d_halo_ref, core_in, core_sum, in_0, in_1, in_2, sum_1, sum_2,
    core_sems, stage_sems, back_sems, back_core_sems, halo_sems,
):
    me, sizes = coordinates(), axis_sizes()

    def partner(axis, step):
        return device_at({**me, axis: lax.rem(me[axis] + sizes[axis] + step, sizes[axis])})

    barrier = pltpu.get_barrier_semaphore()
    greeted = 0
    for axis in ("core", "x", "y", "z"):
        for step in range(1, sizes[axis]):
            pl.semaphore_signal(barrier, inc=1, device_id=partner(axis, step), device_id_type=MESH)
            greeted += 1
    for lat_step, lon_step in ZONE_STEPS:
        pl.semaphore_signal(barrier, inc=1, device_id=neighbour(-lat_step, -lon_step), device_id_type=MESH)
        greeted += 1
    pl.semaphore_wait(barrier, greeted)

    def send(src, dst, sems, number, device):
        copy = pltpu.make_async_remote_copy(
            src_ref=src, dst_ref=dst, send_sem=sems.at[0, number], recv_sem=sems.at[1, number],
            device_id=device, device_id_type=MESH,
        )
        copy.start()
        return copy

    def rows(start, size):
        return pl.ds(pl.multiple_of(start, 16), size)

    pending = []
    counts = [[sizes[axis] for axis in route] for route in ROUTES]
    units = [[CORE_ROWS // n[0], CORE_ROWS // (n[0] * n[1]), CORE_ROWS // (n[0] * n[1] * n[2])] for n in counts]
    spots = [[me[axis] for axis in route] for route in ROUTES]
    other = 1 - me["core"]

    def chunk_of(part, step):
        return lax.rem(spots[part][0] + step, counts[part][0])

    core_copies = {}
    number = 0
    for step in list(range(1, max(counts[0][0], counts[1][0]))) + [0]:
        for part in range(2):
            if step < counts[part][0]:
                size = units[part][0]
                at = chunk_of(part, step) * size
                core_copies[part, step] = send(
                    sums_ref.at[rows(part * PART_ROWS + other * CORE_ROWS + at, size), :],
                    core_in.at[part, rows(at, size), :],
                    core_sems, number, partner("core", 1),
                )
                number += 1
    halo_copies = zone_copies([d_ref], [d_halo_ref], LAYOUTS[:1], 1, halo_sems.at[0], halo_sems.at[1])
    for copy in halo_copies:
        copy.start()

    incoming = (in_0, in_1, in_2)
    numbers = [0]

    def next_number():
        numbers[0] += 1
        return numbers[0] - 1

    stage_copies = {}

    def core_add(part, step):
        core_copies[part, step].wait_recv()
        size = units[part][0]
        at = chunk_of(part, step) * size
        mine = sums_ref[rows(part * PART_ROWS + me["core"] * CORE_ROWS + at, size), :].astype(F32)
        core_sum[part, rows(at, size), :] = (mine + core_in[part, rows(at, size), :].astype(F32)).astype(BF)

    for step in range(1, max(counts[0][0], counts[1][0])):
        for part in range(2):
            if step < counts[part][0]:
                size = units[part][0]
                core_add(part, step)
                stage_copies[part, 0, step] = send(
                    core_sum.at[part, rows(chunk_of(part, step) * size, size), :],
                    in_0.at[part, pl.ds((step - 1) * size, size), :],
                    stage_sems, next_number(), partner(ROUTES[part][0], step),
                )
    for part in range(2):
        core_add(part, 0)

    def add_up(part, stage, own):
        size = units[part][stage]
        total = own.astype(F32)
        for step in range(1, counts[part][stage]):
            stage_copies[part, stage, step].wait_recv()
            total = total + incoming[stage][part, pl.ds((step - 1) * size, size), :].astype(F32)
        return total.astype(BF)

    held = (core_sum, sum_1, sum_2)
    for stage in (1, 2):
        for part in range(2):
            before = units[part][stage - 1]
            if stage == 1:
                own = core_sum[part, rows(spots[part][0] * before, before), :]
            else:
                own = sum_1[part, rows(spots[part][1] * before, before), :]
            held[stage][part, pl.ds(0, before), :] = add_up(part, stage - 1, own)
            size = units[part][stage]
            for step in range(1, counts[part][stage]):
                chunk = lax.rem(spots[part][stage] + step, counts[part][stage])
                stage_copies[part, stage, step] = send(
                    held[stage].at[part, rows(chunk * size, size), :],
                    incoming[stage].at[part, pl.ds((step - 1) * size, size), :],
                    stage_sems, next_number(), partner(ROUTES[part][stage], step),
                )

    def place(part, depth):
        at = part * PART_ROWS + me["core"] * CORE_ROWS
        for stage in range(depth):
            at = at + spots[part][stage] * units[part][stage]
        return at

    back = [0]

    def next_back():
        back[0] += 1
        return back[0] - 1

    back_copies = {}

    def spread_out(part, stage):
        size = units[part][stage]
        mine = out_ref.at[rows(place(part, stage + 1), size), :]
        for step in range(1, counts[part][stage]):
            back_copies[part, stage, step] = send(mine, mine, back_sems, next_back(), partner(ROUTES[part][stage], step))

    def collect(part, stage):
        for step in range(1, counts[part][stage]):
            back_copies[part, stage, step].wait_recv()

    for part in range(2):
        size = units[part][2]
        own = sum_2[part, rows(spots[part][2] * size, size), :]
        out_ref[rows(place(part, 3), size), :] = add_up(part, 2, own)
        spread_out(part, 2)
    for stage in (2, 1):
        for part in range(2):
            collect(part, stage)
            spread_out(part, stage - 1)
    last_copies = []

    def to_core(part, step):
        size = units[part][0]
        spot = lax.rem(spots[part][0] + counts[part][0] - step, counts[part][0])
        piece = out_ref.at[rows(place(part, 0) + spot * size, size), :]
        last_copies.append(send(piece, piece, back_core_sems, len(last_copies), partner("core", 1)))

    for part in range(2):
        to_core(part, 0)
    for step in range(1, max(counts[0][0], counts[1][0])):
        for part in range(2):
            if step < counts[part][0]:
                back_copies[part, 0, step].wait_recv()
                to_core(part, step)
    for copy in last_copies:
        copy.wait()
    for copy in list(core_copies.values()) + list(stage_copies.values()) + list(back_copies.values()):
        copy.wait_send()
    for copy in halo_copies:
        copy.wait()


def sum_all(sums, d_group, collective_id):
    nx, ny, nz = 4, lax.axis_size("lat") // 2, lax.axis_size("lon") // 4
    small = min(nx, ny)
    first = CORE_ROWS - CORE_ROWS // max(nx, ny)
    sum1 = CORE_ROWS // small
    sum2 = CORE_ROWS // (nx * ny)
    firsts = nx + ny
    stage_count = 2 * (nx - 1) + 2 * (ny - 1) + 2 * (nz - 1)
    dma = pltpu.SemaphoreType.DMA
    return pl.pallas_call(
        sum_kernel,
        out_shape=(jax.ShapeDtypeStruct((SUM_ROWS, 128), BF), jax.ShapeDtypeStruct((HALO1, C1), BF)),
        in_specs=[VM, VM],
        out_specs=(VM, VM),
        scratch_shapes=[
            pltpu.VMEM((2, CORE_ROWS, 128), BF),
            pltpu.VMEM((2, CORE_ROWS, 128), BF),
            pltpu.VMEM((2, first, 128), BF),
            pltpu.VMEM((2, sum1, 128), BF),
            pltpu.VMEM((2, sum2, 128), BF),
            pltpu.VMEM((2, sum1, 128), BF),
            pltpu.VMEM((2, sum2, 128), BF),
            dma((2, firsts)),
            dma((2, stage_count)),
            dma((2, stage_count)),
            dma((2, firsts)),
            dma((2, 3)),
        ],
        compiler_params=params(collective_id=collective_id, has_side_effects=True),
    )(sums, d_group)


def spread_matrix():
    wide = np.zeros((256, 12 * 128), np.float32)
    for b in range(12):
        for other in range(6):
            for key in range(12):
                source = other * 23 + b - key + 11
                source = source if source < 128 else source + 256 - SPAN
                wide[source, b * 128 + other * 12 + key] = 1.0
    return wide


def shapes(*entries):
    return tuple(jax.ShapeDtypeStruct(shape, dtype) for shape, dtype in entries)


def local(kernel, out, scratch, *operands, in_specs=None):
    return pl.pallas_call(
        kernel,
        out_shape=shapes(*out),
        in_specs=in_specs or [VM] * len(operands),
        out_specs=(VM,) * len(out),
        scratch_shapes=scratch,
        compiler_params=params(),
    )(*operands)


def shards(
    tokens, cotangent, kinds_one, kinds_two, table_one, table_two, gain_one, gain_merge, gain_two,
    qkv_one, proj_one, merge_weight, qkv_two, proj_two,
):
    maps = jnp.asarray(MAPS)
    spread = jnp.asarray(spread_matrix(), BF)
    gain_one = gain_one.reshape(1, -1)
    gain_merge = gain_merge.reshape(1, -1)
    gain_two = gain_two.reshape(1, -1)

    group, cot_group = local(
        pack_kernel,
        [((GROUP1, C1), BF), ((GROUP2, C2), BF)],
        [pltpu.VMEM((32 * COLS1, C1), F32), pltpu.VMEM((16 * COLS2, C2), F32)],
        maps, tokens, cotangent,
    )
    bias_one, bias_two = local(
        bias_kernel,
        [((4, HEADS1 * BLOCK, 128), F32), ((2, HEADS2 * BLOCK, 128), F32)],
        [pltpu.VMEM((2, 384, 128), F32), pltpu.VMEM((384, 12 * 128), F32)],
        kinds_one, kinds_two, table_one, table_two, spread,
        in_specs=[SM, SM, VM, VM, VM],
    )
    halo_group, halo_cot = halo([group, cot_group], -1, 0)
    act = ((WIN1, C1), BF)
    block_group, x, normed, q, k, v, probs, att = local(
        first_kernel,
        [((GROUP1, C1), BF), act, act, act, act, act, ((8 * HEADS1 * BLOCK, BLOCK), BF), act],
        [],
        maps, group, halo_group, bias_one, gain_one, qkv_one, proj_one,
    )
    (halo_block,) = halo([block_group], -1, 1)
    d_moved, result_group, top_sums = local(
        middle_kernel,
        [((GROUP1, C1), BF), ((GROUP2, C2), BF), ((TOP_ROWS, 128), BF)],
        [pltpu.VMEM((4, WIN2, C1), BF), pltpu.VMEM((4 * C1, C2), F32)],
        maps, block_group, halo_block, cot_group, halo_cot, bias_two, gain_merge, gain_two, merge_weight, qkv_two, proj_two,
    )
    halo_d, halo_result = halo([d_moved, result_group], 1, 2)
    d_group, sums = local(
        last_kernel,
        [((GROUP1, C1), BF), ((SUM_ROWS, 128), BF)],
        [pltpu.VMEM((WIN1, C1), BF) for _ in range(4)],
        maps, d_moved, halo_d, gain_one, qkv_one, proj_one, x, normed, q, k, v, probs, att, top_sums,
    )
    total, halo_tokens = sum_all(sums, d_group, 3)
    return local(
        final_kernel,
        [
            ((2, ROWS2, COLS2 * C2), BF),
            ((2, ROWS1, COLS1 * C1), BF),
            ((C1, 3 * C1), BF),
            ((C1, C1), BF),
            ((4 * C1, C2), BF),
            ((C2, 3 * C2), BF),
            ((C2, C2), BF),
        ],
        [],
        maps, d_group, halo_tokens, result_group, halo_result, total,
    )


def solution(mesh):
    in_specs = (P(None, "lat", "lon"),) * 2 + (P(None, "lat"),) * 2 + (P(),) * 10
    out_specs = (P(None, "lat", "lon"),) * 2 + (P(),) * 5
    return jax.shard_map(shards, mesh=mesh, in_specs=in_specs, out_specs=out_specs, check_vma=False)
```
